512 devices in a mesh: img: 16 (over y, core), row: 32 (over z, x).
Axes of the slice: x: 4, y: 8, z: 8, core: 2. Of those that a mesh axis runs over, the one named last changes fastest.
Arguments:
- lat_pixels: bfloat16 [2048, 256, 320], P(('img', 'row')), parts along dimension 0, may hold values from -40 to 40
- first_gain: float32 [320], replicated, may hold values from 0.1 to 1.9
- first_beta: float32 [320], replicated, may hold values from -3 to 3
- first_kernel: bfloat16 [3, 3, 320, 320], P(None, None, 'row'), may hold values from -0.109375 to 0.109375
- time_shift: float32 [5120], P('img'), parts along dimension 0, may hold values from -3 to 3
- second_gain: float32 [320], replicated, may hold values from 0.1 to 1.9
- second_beta: float32 [320], replicated, may hold values from -3 to 3
- second_kernel: bfloat16 [3, 3, 320, 320], P(None, None, 'row'), may hold values from -0.109375 to 0.109375
- second_bias: float32 [320], replicated, may hold values from -3 to 3
Outputs:
- block_out: bfloat16 [2048, 256, 320], P(('img', 'row')), parts along dimension 0
The draws below stay inside these ranges and needn't reach their ends.
There are 16 independent parts, one for each index of `img`. The reference program is written for one: setup_inputs(seed, part) draws one part's arguments, and reference() takes and returns one part's arrays. A program takes and returns all parts, laid end to end along the dimension named above; an argument that names none is the same for every part. Nothing has to cross between parts.
All inputs are finite; a program needn't handle non-finite values.
Results may differ from the reference program's by a relative error of at most 0.0024.
Values may be sent and summed in bfloat16 or wider, within the bound.
No kernel may reach another device: no remote copies, remote signals or barrier semaphores. Data moves between devices by JAX's collectives and lax.ppermute only.
A program may use at most 64 MiB of HBM per device.

```python
import math
import jax
import jax.numpy as jnp
from jax import lax

CU = 320
GROUPS = 32
WIDTH = 256
HEIGHT = 128


def pixel_draw(key, channels):
    keys = jax.random.split(key, 5)
    heights = jnp.arange(HEIGHT, dtype=jnp.float32)
    rising = jnp.exp(math.log(3.0) * heights / max(HEIGHT - 1, 1))
    row_factor = jnp.exp(jax.random.uniform(keys[0], (HEIGHT,), jnp.float32, 0.0, math.log(3.3)))
    chan_factor = jnp.exp(jax.random.uniform(keys[1], (channels,), jnp.float32, 0.0, math.log(10.0)))
    noise = jax.random.normal(keys[2], (HEIGHT, WIDTH, channels), jnp.float32)
    offset = 0.6 * jax.random.normal(keys[4], (channels,), jnp.float32)
    scale = (rising * row_factor)[:, None, None] * chan_factor[None, None, :] / 6.0
    return jnp.clip(scale * (offset[None, None, :] + noise), -40.0, 40.0)


def draw_lat_pixels(key, part):
    return pixel_draw(jax.random.fold_in(key, 23), CU).astype(jnp.bfloat16)


def levels(own_key, shape, pieces, least, top_value):
    level, own = 1.0, jax.random.fold_in(own_key, 6)
    for axis_at, parts in pieces:
        draws = jnp.exp(jax.random.uniform(jax.random.fold_in(own, axis_at), (parts,), jnp.float32, least / len(pieces), top_value / len(pieces)))
        level = level * jnp.repeat(draws, shape[axis_at] // parts).reshape([-1 if axis == axis_at else 1 for axis in range(len(shape))])
    return level


def centred(stream_key, dims, scale, limit, shards=(), kind=jnp.bfloat16):
    entries = scale * jax.random.normal(stream_key, dims, jnp.float32)
    if shards:
        entries = entries * levels(stream_key, dims, shards, -0.22, 0.18)
    return jnp.clip(entries, -limit, limit).astype(kind)


def setup_inputs(seed: int = 0, part: int = 0) -> dict:
    arg_keys = jax.random.split(jax.random.key(seed), 10)
    part_keys = jax.random.split(jax.random.fold_in(arg_keys[9], part), 10)
    lat_pixels = draw_lat_pixels(jax.random.fold_in(jax.random.fold_in(arg_keys[9], part), 71), part)
    first_gain = jnp.clip(1.0 + 0.18 * jax.random.normal(arg_keys[1], (CU,), jnp.float32), 0.1, 1.9)
    first_beta = centred(arg_keys[2], (CU,), 0.5, 3.0, (), jnp.float32)
    first_kernel = centred(arg_keys[3], (3, 3, CU, CU), (9 * CU) ** -0.5, 0.109375, ((2, 32),))
    time_shift = centred(part_keys[4], (CU,), 0.5, 3.0, (), jnp.float32)
    second_gain = jnp.clip(1.0 + 0.18 * jax.random.normal(arg_keys[5], (CU,), jnp.float32), 0.1, 1.9)
    second_beta = centred(arg_keys[6], (CU,), 0.5, 3.0, (), jnp.float32)
    second_kernel = centred(arg_keys[7], (3, 3, CU, CU), (9 * CU) ** -0.5, 0.109375, ((2, 32),))
    second_bias = centred(arg_keys[8], (CU,), 0.5, 3.0, (), jnp.float32)
    return dict(lat_pixels=lat_pixels, first_gain=first_gain, first_beta=first_beta, first_kernel=first_kernel, time_shift=time_shift, second_gain=second_gain, second_beta=second_beta, second_kernel=second_kernel, second_bias=second_bias)


epsilon = 1e-06

def activate(pixels, gain, beta):
    values = pixels.astype(jnp.float32)
    channels = values.shape[-1]
    grouped = values.reshape(-1, GROUPS, channels // GROUPS)
    center = lax.optimization_barrier(jnp.mean(grouped, axis=(0, 2)))
    spread = lax.optimization_barrier(jnp.mean(jnp.square(grouped - center[None, :, None]), axis=(0, 2)))
    normed = (grouped - center[None, :, None]) * lax.rsqrt(spread + epsilon)[None, :, None]
    normed = normed.reshape(values.shape) * gain.astype(jnp.float32) + beta.astype(jnp.float32)
    return jax.nn.silu(normed).astype(jnp.bfloat16)

def band_conv(padded, kernel):
    rows_out = padded.shape[0] - 2
    width_out = padded.shape[1] - 2
    count = kernel.shape[2]
    total = jnp.zeros((rows_out * width_out, kernel.shape[3]), jnp.float32)
    for tap_row in range(3):
        band = padded[tap_row:tap_row + rows_out]
        columns = jnp.concatenate([band[:, offset:offset + width_out] for offset in range(3)], axis=-1)
        columns = columns.reshape(rows_out * width_out, 3 * count)
        total = total + jnp.dot(columns, kernel[tap_row].reshape(3 * count, -1), preferred_element_type=jnp.float32)
    return total

def norm_conv(pixels, gain, beta, kernel):
    active = activate(pixels, gain, beta)
    padded = jnp.pad(active, ((1, 1), (1, 1), (0, 0)))
    return band_conv(padded, kernel).reshape(pixels.shape)

def reference(lat_pixels, first_gain, first_beta, first_kernel, time_shift, second_gain, second_beta, second_kernel, second_bias):
    hidden = (norm_conv(lat_pixels, first_gain, first_beta, first_kernel) + time_shift.astype(jnp.float32)).astype(jnp.bfloat16)
    hidden = lax.optimization_barrier(hidden)
    second = norm_conv(hidden, second_gain, second_beta, second_kernel)
    return (lat_pixels.astype(jnp.float32) + second + second_bias.astype(jnp.float32)).astype(jnp.bfloat16)
```

```python
import functools

import jax
import jax.numpy as jnp
from jax import lax
from jax.experimental import pallas as pl
from jax.experimental.pallas import tpu as pltpu
from jax.sharding import Mesh
from jax.sharding import PartitionSpec as P

GROUPS = 32
PER = 10
CU = 320
WIDTH = 256
TAPS = 9
SLABS = TAPS * PER
PAIRS = SLABS // 2
CROWS = 23
CHUNK = 120
DEPTH = SLABS * GROUPS
ROWK = 3 * CU
ROW = ("row_0", "row_1")
IMG_ROW = ("y", "core", "row_0", "row_1")
EPS = 1e-06

f32 = jnp.float32
bf16 = jnp.bfloat16
WHOLE = pl.BlockSpec(memory_space=pltpu.VMEM)
SCALARS = pl.BlockSpec(memory_space=pltpu.SMEM)
PARAMS = pltpu.CompilerParams(vmem_limit_bytes=48 * 1024 * 1024)


def widen(ref, at, values):
    ref[at : at + CU, :] = values[:, 0:128]
    ref[at + CU : at + 2 * CU, :] = values[:, 128:256]


def slab_of(ref, j, row=0):
    at = row * 2 * CU + j
    halves = [ref[pl.ds(at + n * CU, GROUPS, stride=PER), :] for n in range(2)]
    return jnp.concatenate(halves, axis=1)


def same_slab(ref, j):
    half = ref[pl.ds(j, GROUPS, stride=PER), :]
    return jnp.concatenate([half, half], axis=1)


def local_moments(values, rows):
    total = jnp.zeros((GROUPS, WIDTH), f32)
    for h in range(rows):
        for j in range(PER):
            total += slab_of(values, j, h)
    mean = jnp.sum(total, axis=1, keepdims=True) * (1.0 / (rows * PER * WIDTH))
    off = jnp.zeros((GROUPS, WIDTH), f32)
    for h in range(rows):
        for j in range(PER):
            d = slab_of(values, j, h) - mean
            off += d * d
    return mean, jnp.sum(off, axis=1, keepdims=True)


def turned(column):
    return jnp.transpose(jnp.broadcast_to(column, (column.shape[0], 128)))


def in_three(v):
    hi = v.astype(bf16).astype(f32)
    rest = v - hi
    mid = rest.astype(bf16).astype(f32)
    return hi, mid, rest - mid


def prep_kernel(core_ref, x_ref, w_ref, ch_ref, wide, flat, chunk):
    core = core_ref[0]
    for h in range(4):
        widen(wide, h * 2 * CU, x_ref[h].astype(f32))
    fill_chunk(core, w_ref, flat, chunk)
    mean, off = local_moments(wide, 4)
    for k, col in enumerate((mean, off)):
        row = turned(col)[0:1, :]
        for n, piece in enumerate(in_three(row)):
            at = SLABS + CROWS + 3 * k + n
            chunk[at : at + 1, 0:GROUPS] = piece
    whole = chunk[...].astype(bf16)
    for d in range(GROUPS):
        ch_ref[d] = whole


def fill_chunk(core, w_ref, flat, chunk):
    for p in range(3):
        for j in range(PER):
            at = (p * PER + j) * 3
            flat[at : at + 3, 0:CU] = w_ref[p, j].astype(f32)
    chunk[...] = jnp.zeros((CHUNK, 128), f32)
    first = core == 0
    chunk[0:SLABS, :] = jnp.where(first, flat[0:SLABS, 0:128], flat[0:SLABS, 128:256])
    for c in range(2):
        t0 = (CROWS - 1) * c
        lo = flat[t0 : t0 + CROWS, 256:384]
        hi = pltpu.roll(flat[PAIRS + t0 : PAIRS + t0 + CROWS, 256:384], 64, 1)
        lane = lax.broadcasted_iota(jnp.int32, (CROWS, 128), 1)
        both = jnp.where(lane < 64, lo, hi)

        @pl.when(core == c)
        def _():
            chunk[SLABS : SLABS + CROWS, :] = both


def prep2_kernel(core_ref, w_ref, ch_ref, flat, chunk):
    fill_chunk(core_ref[0], w_ref, flat, chunk)
    whole = chunk[...].astype(bf16)
    for d in range(GROUPS):
        ch_ref[d] = whole


def prep(core, x, w):
    return pl.pallas_call(
        prep_kernel,
        out_shape=jax.ShapeDtypeStruct((GROUPS, CHUNK, 128), bf16),
        in_specs=[SCALARS, WHOLE, WHOLE],
        out_specs=WHOLE,
        scratch_shapes=[
            pltpu.VMEM((8 * CU, 128), f32),
            pltpu.VMEM((96, 384), f32),
            pltpu.VMEM((CHUNK, 128), f32),
        ],
        compiler_params=PARAMS,
        name="prep",
    )(core, x, w)


def prep2(core, w):
    return pl.pallas_call(
        prep2_kernel,
        out_shape=jax.ShapeDtypeStruct((GROUPS, CHUNK, 128), bf16),
        in_specs=[SCALARS, WHOLE],
        out_specs=WHOLE,
        scratch_shapes=[pltpu.VMEM((96, 384), f32), pltpu.VMEM((CHUNK, 128), f32)],
        compiler_params=PARAMS,
        name="prep2",
    )(core, w)


def column_of(row):
    return jnp.transpose(jnp.broadcast_to(row, (128, row.shape[1])))


def combine(means, offs, count):
    n = means.shape[0]
    center = jnp.sum(means, axis=0, keepdims=True) * (1.0 / n)
    d = means - center
    spread = (jnp.sum(offs, axis=0, keepdims=True) + count * jnp.sum(d * d, axis=0, keepdims=True)) * (
        1.0 / (n * count)
    )
    inv = lax.rsqrt(spread + EPS)
    return column_of(center), column_of(inv)


def activate(flags_ref, rows, center, inv, gain_ref, beta_ref, cols, wide, act_ref):
    gains, betas = cols
    gains[...] = column_of(gain_ref[...])
    betas[...] = column_of(beta_ref[...])
    two = lambda a: jnp.concatenate([a, a], axis=1)
    center, inv = two(center), two(inv)
    lane = lax.broadcasted_iota(jnp.int32, (GROUPS, WIDTH), 1)
    for h in range(6):
        widen(wide, 0, rows(h).astype(f32))
        for j in range(PER):
            v = (slab_of(wide, j) - center) * inv
            v = v * same_slab(gains, j) + same_slab(betas, j)
            v = v / (1.0 + jnp.exp(-v))
            if h == 0:
                v = jnp.where(flags_ref[1] == 0, 0.0, v)
            if h == 5:
                v = jnp.where(flags_ref[2] == 0, 0.0, v)
            left = jnp.where(lane == 0, 0.0, pltpu.roll(v, 1, 1))
            right = jnp.where(lane == WIDTH - 1, 0.0, pltpu.roll(v, WIDTH - 1, 1))
            at = h * ROWK + j * 3 * GROUPS
            act_ref[at : at + GROUPS, :] = left.astype(bf16)
            act_ref[at + GROUPS : at + 2 * GROUPS, :] = v.astype(bf16)
            act_ref[at + 2 * GROUPS : at + 3 * GROUPS, :] = right.astype(bf16)


def pick_rows(top_ref, mid_ref, bot_ref):
    def rows(h):
        return top_ref[0] if h == 0 else bot_ref[0] if h == 5 else mid_ref[h - 1]

    return rows


def norm1_kernel(flags_ref, g_ref, top_ref, mid_ref, bot_ref, gain_ref, beta_ref, act_ref, gains, betas, wide):
    tail = g_ref[:, CHUNK - 8 : CHUNK, :].astype(f32)
    piece = lambda n: tail[:, n, 0:GROUPS]
    means = piece(1) + piece(2) + piece(3)
    offs = piece(4) + piece(5) + piece(6)
    center, inv = combine(means, offs, 4.0 * PER * WIDTH)
    activate(flags_ref, pick_rows(top_ref, mid_ref, bot_ref), center, inv, gain_ref, beta_ref, (gains, betas), wide, act_ref)


def norm2_kernel(flags_ref, s_ref, top_ref, mid_ref, bot_ref, gain_ref, beta_ref, act_ref, gains, betas, wide):
    both = s_ref[:, 0, :]
    center, inv = combine(both[:, 0:GROUPS], both[:, GROUPS : 2 * GROUPS], 4.0 * PER * WIDTH)
    activate(flags_ref, pick_rows(top_ref, mid_ref, bot_ref), center, inv, gain_ref, beta_ref, (gains, betas), wide, act_ref)


def norm(kernel, flags, stats, top, mid, bot, gain, beta):
    return pl.pallas_call(
        kernel,
        out_shape=jax.ShapeDtypeStruct((6 * ROWK, WIDTH), bf16),
        in_specs=[SCALARS] + [WHOLE] * 6,
        out_specs=WHOLE,
        scratch_shapes=[pltpu.VMEM((CU, 128), f32), pltpu.VMEM((CU, 128), f32), pltpu.VMEM((2 * CU, 128), f32)],
        compiler_params=PARAMS,
        name=kernel.__name__,
    )(flags, stats, top, mid, bot, gain.reshape(1, CU), beta.reshape(1, CU))


def gather_half(core, g_ref, wide, w):
    for d in range(GROUPS):
        wide[d * CHUNK : (d + 1) * CHUNK, :] = g_ref[d].astype(f32)
    lanes = pl.ds(pl.multiple_of(core * 128, 128), 128)
    for m in range(SLABS):
        v = wide[pl.ds(m, GROUPS, stride=CHUNK), :]
        w[m * GROUPS : (m + 1) * GROUPS, lanes] = v.astype(bf16)
    t0 = core * (CROWS - 1)
    for t in range(CROWS):
        v = wide[pl.ds(SLABS + t, GROUPS, stride=CHUNK), :]
        at = pl.multiple_of((t0 + t) * GROUPS, GROUPS)
        w[pl.ds(at, GROUPS), 256:384] = v.astype(bf16)
        w[pl.ds(at + PAIRS * GROUPS, GROUPS), 256:384] = pltpu.roll(v, 64, 1).astype(bf16)


def weights(flags_ref, own_ref, other_ref, wide, w, wt):
    core = flags_ref[0]
    gather_half(core, own_ref, wide, w)
    gather_half(1 - core, other_ref, wide, w)
    for p in range(3):
        wt[p] = jnp.transpose(w[p * ROWK : (p + 1) * ROWK, 0:CU])


def conv_row(h, act_ref, wt):
    total = None
    for p in range(3):
        part = jnp.dot(
            wt[p], act_ref[(h + p) * ROWK : (h + p + 1) * ROWK, :], preferred_element_type=f32
        )
        total = part if total is None else total + part
    return total


def conv1_kernel(flags_ref, own_ref, other_ref, act_ref, shift_ref, hid_ref, st_ref, wide, w, wt, full):
    weights(flags_ref, own_ref, other_ref, wide, w, wt)
    shift = column_of(shift_ref[...])
    shift = jnp.concatenate([shift, shift], axis=1)
    for h in range(4):
        row = (conv_row(h, act_ref, wt) + shift).astype(bf16)
        hid_ref[h] = row
        widen(full, h * 2 * CU, row.astype(f32))
    mean, off = local_moments(full, 4)
    line = turned(jnp.concatenate([mean, off], axis=0))[0:1, :]
    line = jnp.concatenate([line, jnp.zeros((1, 64), f32)], axis=1)
    for d in range(GROUPS):
        st_ref[d] = line


CONV_SCRATCH = [
    pltpu.VMEM((GROUPS * CHUNK, 128), f32),
    pltpu.VMEM((DEPTH, 384), bf16),
    pltpu.VMEM((3, CU, ROWK), bf16),
]


def conv1(flags, own, other, act, shift):
    return pl.pallas_call(
        conv1_kernel,
        out_shape=(
            jax.ShapeDtypeStruct((4, CU, WIDTH), bf16),
            jax.ShapeDtypeStruct((GROUPS, 1, 128), f32),
        ),
        in_specs=[SCALARS] + [WHOLE] * 4,
        out_specs=(WHOLE, WHOLE),
        scratch_shapes=CONV_SCRATCH + [pltpu.VMEM((8 * CU, 128), f32)],
        compiler_params=PARAMS,
        name="conv1",
    )(flags, own, other, act, shift.reshape(1, CU))


def conv2_kernel(flags_ref, own_ref, other_ref, act_ref, bias_ref, x_ref, out_ref, wide, w, wt):
    weights(flags_ref, own_ref, other_ref, wide, w, wt)
    bias = column_of(bias_ref[...])
    bias = jnp.concatenate([bias, bias], axis=1)
    for h in range(4):
        out_ref[h] = (x_ref[h].astype(f32) + conv_row(h, act_ref, wt) + bias).astype(bf16)


def conv2(flags, own, other, act, bias, x):
    return pl.pallas_call(
        conv2_kernel,
        out_shape=jax.ShapeDtypeStruct((4, CU, WIDTH), bf16),
        in_specs=[SCALARS] + [WHOLE] * 5,
        out_specs=WHOLE,
        scratch_shapes=CONV_SCRATCH,
        compiler_params=PARAMS,
        name="conv2",
    )(flags, own, other, act, bias.reshape(1, CU), x)


def to_all(chunks):
    return lax.all_to_all(chunks, ROW, 0, 0, tiled=True)


def swapped(chunks):
    return lax.ppermute(chunks, "core", [(0, 1), (1, 0)])


def edges(rows):
    count = lax.axis_size(ROW)
    above = lax.ppermute(rows[3:4], ROW, [(i, i + 1) for i in range(count - 1)])
    below = lax.ppermute(rows[0:1], ROW, [(i + 1, i) for i in range(count - 1)])
    return above, below


def shards(
    lat_pixels,
    first_gain,
    first_beta,
    first_kernel,
    time_shift,
    second_gain,
    second_beta,
    second_kernel,
    second_bias,
):
    x = lat_pixels.transpose(0, 2, 1)
    place = lax.axis_index(ROW)
    last = lax.axis_size(ROW) - 1
    flags = jnp.stack(
        [lax.axis_index("core"), (place > 0).astype(jnp.int32), (place < last).astype(jnp.int32)]
    ).astype(jnp.int32)
    ch1 = prep(flags, x, first_kernel.transpose(0, 2, 1, 3))
    ch2 = prep2(flags, second_kernel.transpose(0, 2, 1, 3))
    own1 = to_all(ch1)
    own2 = to_all(ch2)
    above, below = edges(x)
    other1 = swapped(own1)
    act = norm(norm1_kernel, flags, own1, above, x, below, first_gain, first_beta)
    hidden, st = conv1(flags, own1, other1, act, time_shift)
    habove, hbelow = edges(hidden)
    stats = to_all(st)
    other2 = swapped(own2)
    act2 = norm(norm2_kernel, flags, stats, habove, hidden, hbelow, second_gain, second_beta)
    out = conv2(flags, own2, other2, act2, second_bias, x)
    return out.transpose(0, 2, 1)


def solution(mesh):
    split = Mesh(mesh.devices.reshape(mesh.shape["img"] // 2, 2, 8, 4), ("y", "core", "row_0", "row_1"))
    placed = (
        P(IMG_ROW, None, None),
        P(),
        P(),
        P(None, None, ROW, None),
        P(("y", "core")),
        P(),
        P(),
        P(None, None, ROW, None),
        P(),
    )
    return jax.shard_map(
        shards, mesh=split, in_specs=placed, out_specs=P(IMG_ROW, None, None), check_vma=False
    )
```

```python
import jax
import jax.numpy as jnp
from jax import lax
from jax.experimental import pallas as pl
from jax.experimental.pallas import tpu as pltpu
from jax.sharding import Mesh
from jax.sharding import PartitionSpec as P

GROUPS = 32
PER = 10
CU = 320
WIDTH = 256
TAPS = 9
SLABS = TAPS * PER
PAIRS = SLABS // 2
CROWS = 23
CHUNK = 120
ZS, XS = 8, 4
LOCAL = 4.0 * PER * WIDTH
DEPTH = SLABS * GROUPS
ROWK = 1024
ROW = ("row_0", "row_1")
IMG_ROW = ("y", "core", "row_0", "row_1")
EPS = 1e-06

f32 = jnp.float32
bf16 = jnp.bfloat16
ANYWHERE = pl.BlockSpec(memory_space=pl.ANY)
FAR = pl.BlockSpec(memory_space=pltpu.HBM)
WHOLE = pl.BlockSpec(memory_space=pltpu.VMEM)
SCALARS = pl.BlockSpec(memory_space=pltpu.SMEM)
PARAMS = pltpu.CompilerParams(vmem_limit_bytes=24 * 1024 * 1024)


def far(array):
    return pltpu.with_memory_space_constraint(array, pltpu.HBM)


def near(*arrays):
    return [pltpu.with_memory_space_constraint(a, pltpu.VMEM) for a in arrays]


def cost(us):
    return pl.CostEstimate(flops=int(us * 2e8), bytes_accessed=1 << 20, transcendentals=0)


def widen(ref, at, values):
    ref[at : at + CU, :] = values[:, 0:128]
    ref[at + CU : at + 2 * CU, :] = values[:, 128:256]


def slab_of(ref, j, row=0):
    at = row * 2 * CU + j
    halves = [ref[pl.ds(at + n * CU, GROUPS, stride=PER), :] for n in range(2)]
    return jnp.concatenate(halves, axis=1)


def same_slab(ref, j):
    half = ref[pl.ds(j, GROUPS, stride=PER), :]
    return jnp.concatenate([half, half], axis=1)


def local_moments(values, rows):
    total = jnp.zeros((GROUPS, WIDTH), f32)
    for h in range(rows):
        for j in range(PER):
            total += slab_of(values, j, h)
    mean = jnp.sum(total, axis=1, keepdims=True) * (1.0 / (rows * PER * WIDTH))
    off = jnp.zeros((GROUPS, WIDTH), f32)
    for h in range(rows):
        for j in range(PER):
            d = slab_of(values, j, h) - mean
            off += d * d
    return mean, jnp.sum(off, axis=1, keepdims=True)


def turned(column):
    return jnp.transpose(jnp.broadcast_to(column, (column.shape[0], 128)))


def in_three(v):
    hi = v.astype(bf16).astype(f32)
    rest = v - hi
    mid = rest.astype(bf16).astype(f32)
    return hi, mid, rest - mid


def prep_kernel(
    flags_ref, x_hbm, w_hbm, w2_hbm, ch_ref, x_ref, w_ref, w2_ref, wide, flat, chunk, x_sem, w_sem, w2_sem
):
    core = flags_ref[0]
    get_x = pltpu.make_async_copy(x_hbm, x_ref, x_sem)
    get_w = pltpu.make_async_copy(w_hbm, w_ref, w_sem)
    get_w2 = pltpu.make_async_copy(w2_hbm, w2_ref, w2_sem)
    get_w.start()
    get_w2.start()
    get_x.start()
    get_w2.wait()
    fill_chunk(core, w2_ref, flat, chunk)
    whole = chunk[...].astype(bf16)
    for d in range(ZS):
        ch_ref[d, CHUNK : 2 * CHUNK] = whole
    get_w.wait()
    fill_chunk(core, w_ref, flat, chunk)
    get_x.wait()
    for h in range(4):
        widen(wide, h * 2 * CU, x_ref[h].astype(f32))
    mean, off = local_moments(wide, 4)
    rows = [turned(col)[0:1, :] for col in (mean, off)]
    put_stats(rows, chunk)
    whole = chunk[...].astype(bf16)
    for d in range(ZS):
        ch_ref[d, 0:CHUNK] = whole


def put_stats(rows, chunk):
    for k, row in enumerate(rows):
        for n, piece in enumerate(in_three(row[:, 0:GROUPS])):
            at = SLABS + CROWS + 3 * k + n
            chunk[at : at + 1, 0:GROUPS] = piece


def got_stats(tail):
    piece = lambda n: tail[:, n, 0:GROUPS]
    return piece(1) + piece(2) + piece(3), piece(4) + piece(5) + piece(6)


def pooled(means, offs, count):
    n = means.shape[0]
    mean = jnp.sum(means, axis=0, keepdims=True) * (1.0 / n)
    d = means - mean
    return mean, jnp.sum(offs, axis=0, keepdims=True) + count * jnp.sum(d * d, axis=0, keepdims=True)


def middle_kernel(g_ref, above_ref, below_ref, xch_ref, w2_ref, tail):
    rows = pooled(*got_stats(g_ref[:, CHUNK - 8 : CHUNK, :].astype(f32)), LOCAL)
    tail[...] = g_ref[0, 0:CHUNK, :].astype(f32)
    put_stats(rows, tail)
    first = tail[...].astype(bf16)
    for d in range(XS):
        xch_ref[d, 0] = first
        for z in range(1, ZS):
            xch_ref[d, z] = g_ref[z, 0:CHUNK, :]
    for z in range(ZS):
        w2_ref[z] = g_ref[z, CHUNK : 2 * CHUNK, :]


def middle(got, above, below):
    return pl.pallas_call(
        middle_kernel,
        out_shape=(
            jax.ShapeDtypeStruct((XS, ZS, CHUNK, 128), bf16),
            pltpu.VMEM((ZS, CHUNK, 128), bf16),
        ),
        in_specs=[WHOLE, ANYWHERE, ANYWHERE],
        out_specs=(WHOLE, WHOLE),
        scratch_shapes=[pltpu.VMEM((CHUNK, 128), f32)],
        compiler_params=PARAMS,
        cost_estimate=cost(1),
        name="middle",
    )(got, above, below)


def join_kernel(flags_ref, own_ref, a_ref, b_ref, c_ref, after_ref, out_ref):
    x = flags_ref[3]
    for s, ref in enumerate((own_ref, a_ref, b_ref, c_ref)):
        at = (x + XS - s) % XS
        for z in range(ZS):
            out_ref[z * XS + at] = ref[z]


def join(flags, pieces, after):
    return pl.pallas_call(
        join_kernel,
        out_shape=pltpu.VMEM((GROUPS, CHUNK, 128), bf16),
        in_specs=[SCALARS] + [WHOLE] * 4 + [ANYWHERE],
        out_specs=WHOLE,
        compiler_params=PARAMS,
        cost_estimate=cost(1),
        name="join",
    )(flags, *near(*pieces), after)


def fill_chunk(core, w_ref, flat, chunk):
    for p in range(3):
        for j in range(PER):
            at = (p * PER + j) * 3
            flat[at : at + 3, 0:CU] = w_ref[p, j].astype(f32)
    chunk[...] = jnp.zeros((CHUNK, 128), f32)
    first = core == 0
    chunk[0:SLABS, :] = jnp.where(first, flat[0:SLABS, 0:128], flat[0:SLABS, 128:256])
    for c in range(2):
        t0 = (CROWS - 1) * c
        lo = flat[t0 : t0 + CROWS, 256:384]
        hi = pltpu.roll(flat[PAIRS + t0 : PAIRS + t0 + CROWS, 256:384], 64, 1)
        lane = lax.broadcasted_iota(jnp.int32, (CROWS, 128), 1)
        both = jnp.where(lane < 64, lo, hi)

        @pl.when(core == c)
        def _():
            chunk[SLABS : SLABS + CROWS, :] = both


def prep(flags, *arrays):
    arrays = [far(a) for a in arrays]
    return pl.pallas_call(
        prep_kernel,
        out_shape=jax.ShapeDtypeStruct((ZS, 2 * CHUNK, 128), bf16),
        in_specs=[SCALARS] + [FAR] * 3,
        out_specs=WHOLE,
        scratch_shapes=[
            pltpu.VMEM((4, CU, WIDTH), bf16),
            pltpu.VMEM((3, PER, 3, CU), bf16),
            pltpu.VMEM((3, PER, 3, CU), bf16),
            pltpu.VMEM((8 * CU, 128), f32),
            pltpu.VMEM((96, 384), f32),
            pltpu.VMEM((CHUNK, 128), f32),
            pltpu.SemaphoreType.DMA,
            pltpu.SemaphoreType.DMA,
            pltpu.SemaphoreType.DMA,
        ],
        compiler_params=PARAMS,
        cost_estimate=cost(3),
        name="prep",
    )(flags, *arrays)


def column_of(row):
    return jnp.transpose(jnp.broadcast_to(row, (128, row.shape[1])))


def combine(means, offs, count):
    center, off = pooled(means, offs, count)
    inv = lax.rsqrt(off * (1.0 / (means.shape[0] * count)) + EPS)
    return column_of(center), column_of(inv)


def activate(flags_ref, rows, center, inv, gain_ref, beta_ref, cols, wide, act_ref):
    gains, betas = cols
    gains[...] = column_of(gain_ref[...])
    betas[...] = column_of(beta_ref[...])
    two = lambda a: jnp.concatenate([a, a], axis=1)
    center, inv = two(center), two(inv)
    lane = lax.broadcasted_iota(jnp.int32, (GROUPS, WIDTH), 1)
    for h in (1, 2, 3, 4, 0, 5):
        act_ref[h * ROWK + 3 * CU : (h + 1) * ROWK, :] = jnp.zeros((ROWK - 3 * CU, WIDTH), bf16)
        widen(wide, 0, rows(h).astype(f32))
        for j in range(PER):
            v = (slab_of(wide, j) - center) * inv
            v = v * same_slab(gains, j) + same_slab(betas, j)
            v = v / (1.0 + jnp.exp(-v))
            if h == 0:
                v = jnp.where(flags_ref[1] == 0, 0.0, v)
            if h == 5:
                v = jnp.where(flags_ref[2] == 0, 0.0, v)
            left = jnp.where(lane == 0, 0.0, pltpu.roll(v, 1, 1))
            right = jnp.where(lane == WIDTH - 1, 0.0, pltpu.roll(v, WIDTH - 1, 1))
            at = h * ROWK + j * 3 * GROUPS
            act_ref[at : at + GROUPS, :] = left.astype(bf16)
            act_ref[at + GROUPS : at + 2 * GROUPS, :] = v.astype(bf16)
            act_ref[at + 2 * GROUPS : at + 3 * GROUPS, :] = right.astype(bf16)


def fetched(fars, here, sems):
    copies = [pltpu.make_async_copy(far_ref, here.at[n], sems.at[n]) for n, far_ref in enumerate(fars)]
    for copy in copies:
        copy.start()

    def get(n):
        copies[n].wait()
        return here[n]

    return get


def norm1_kernel(
    flags_ref, g_ref, top_hbm, mid_ref, bot_hbm, gain_ref, beta_ref, act_ref, wt_ref, gains, betas, wide, many, here, sems
):
    edge = fetched((top_hbm.at[0], bot_hbm.at[0]), here, sems)
    own_block(g_ref, many, wt_ref)
    center, inv = combine(*got_stats(g_ref[:, 0, CHUNK - 8 : CHUNK, :].astype(f32)), ZS * LOCAL)
    rows = lambda h: mid_ref[h - 1] if 0 < h < 5 else edge(int(h == 5))
    activate(flags_ref, rows, center, inv, gain_ref, beta_ref, (gains, betas), wide, act_ref)


def norm2_kernel(
    flags_ref, s_ref, top_ref, mid_hbm, bot_ref, gain_ref, beta_ref, act_ref, gains, betas, wide, here, sems
):
    middle_row = fetched([mid_hbm.at[h] for h in range(4)], here, sems)
    both = s_ref[:, 0, :]
    center, inv = combine(both[:, 0:GROUPS], both[:, GROUPS : 2 * GROUPS], LOCAL)
    rows = lambda h: middle_row(h - 1) if 0 < h < 5 else (bot_ref if h else top_ref)[0]
    activate(flags_ref, rows, center, inv, gain_ref, beta_ref, (gains, betas), wide, act_ref)


NORM_SCRATCH = [
    pltpu.VMEM((CU, 128), f32),
    pltpu.VMEM((CU, 128), f32),
    pltpu.VMEM((2 * CU, 128), f32),
]
MANY = pltpu.VMEM((GROUPS * CHUNK, 128), f32)
ACT = pltpu.VMEM((6 * ROWK, WIDTH), bf16)


def rows_here(n):
    return [pltpu.VMEM((n, CU, WIDTH), bf16), pltpu.SemaphoreType.DMA((n,))]


def norm1(flags, own, top, mid, bot, gain, beta):
    return pl.pallas_call(
        norm1_kernel,
        out_shape=(ACT, pltpu.VMEM((128, 3 * ROWK), bf16)),
        in_specs=[SCALARS, WHOLE, FAR, WHOLE, FAR, WHOLE, WHOLE],
        out_specs=(WHOLE, WHOLE),
        scratch_shapes=NORM_SCRATCH + [MANY] + rows_here(2),
        compiler_params=PARAMS,
        cost_estimate=cost(3),
        name="norm1",
    )(flags, *near(own), far(top), mid, far(bot), gain.reshape(1, CU), beta.reshape(1, CU))


def norm2(flags, stats, top, mid, bot, gain, beta):
    return pl.pallas_call(
        norm2_kernel,
        out_shape=ACT,
        in_specs=[SCALARS, WHOLE, WHOLE, FAR, WHOLE, WHOLE, WHOLE],
        out_specs=WHOLE,
        scratch_shapes=NORM_SCRATCH + rows_here(4),
        compiler_params=PARAMS,
        cost_estimate=cost(2),
        name="norm2",
    )(flags, stats, top, far(mid), bot, gain.reshape(1, CU), beta.reshape(1, CU))


def shard_at(g_ref, d, rows):
    part = g_ref[d, rows, :] if len(g_ref.shape) == 3 else g_ref[d % XS, d // XS, rows, :]
    return part.astype(f32)


def spread_out(g_ref, many):
    for d in range(GROUPS):
        many[d * CHUNK : (d + 1) * CHUNK, :] = shard_at(g_ref, d, slice(0, CHUNK))


def block(many):
    out = []
    for p in range(3):
        slabs = [many[pl.ds(p * 30 + m, GROUPS, stride=CHUNK), :].astype(bf16) for m in range(30)]
        slabs.append(jnp.zeros((ROWK - 3 * CU, 128), bf16))
        out.append(jnp.transpose(jnp.concatenate(slabs, axis=0)))
    return out


def own_block(g_ref, many, wt_ref):
    spread_out(g_ref, many)
    for p, part in enumerate(block(many)):
        wt_ref[:, p * ROWK : (p + 1) * ROWK] = part


def rest_of(core, many, w):
    t0 = core * (CROWS - 1)
    for t in range(CROWS):
        v = many[pl.ds(SLABS + t, GROUPS, stride=CHUNK), :]
        at = pl.multiple_of((t0 + t) * GROUPS, GROUPS)
        w[pl.ds(at, GROUPS), :] = v.astype(bf16)
        w[pl.ds(at + PAIRS * GROUPS, GROUPS), :] = pltpu.roll(v, 64, 1).astype(bf16)


def rest_turned(w, wt):
    for p in range(3):
        part = jnp.concatenate([w[p * 3 * CU : (p + 1) * 3 * CU, :], jnp.zeros((ROWK - 3 * CU, 128), bf16)], axis=0)
        wt[256:CU, p * ROWK : (p + 1) * ROWK] = jnp.transpose(part)[0:64, :]


def rows_of(core):
    return pl.ds(pl.multiple_of(core * 128, 128), 128)


def conv_row(h, act_ref, wt):
    return jnp.dot(wt[...], act_ref[h * ROWK : (h + 3) * ROWK, :], preferred_element_type=f32)


def all_weights(flags_ref, own_ref, wto_ref, other_ref, many, many2, w, wt):
    core = flags_ref[0]
    for d in range(GROUPS):
        many2[d * 32 : (d + 1) * 32, :] = shard_at(own_ref, d, slice(CHUNK - 32, CHUNK))
    t0 = core * (CROWS - 1)
    for t in range(CROWS):
        v = many2[pl.ds(2 + t, GROUPS, stride=32), :]
        at = pl.multiple_of((t0 + t) * GROUPS, GROUPS)
        w[pl.ds(at, GROUPS), :] = v.astype(bf16)
        w[pl.ds(at + PAIRS * GROUPS, GROUPS), :] = pltpu.roll(v, 64, 1).astype(bf16)
    spread_out(other_ref, many)
    rest_of(1 - core, many, w)
    rest_turned(w, wt)
    wt[rows_of(core), :] = wto_ref[...]
    for p, part in enumerate(block(many)):
        wt[rows_of(1 - core), p * ROWK : (p + 1) * ROWK] = part


def conv1_kernel(
    flags_ref, own_ref, wto_ref, other_ref, act_ref, shift_ref, hid_hbm, first_hbm, last_hbm, st_ref, many, many2, w, wt, full, hid, sems
):
    all_weights(flags_ref, own_ref, wto_ref, other_ref, many, many2, w, wt)
    shift = column_of(shift_ref[...])
    shift = jnp.concatenate([shift, shift], axis=1)
    for h in range(4):
        row = (conv_row(h, act_ref, wt) + shift).astype(bf16)
        hid[h] = row
        widen(full, h * 2 * CU, row.astype(f32))
    puts = [
        pltpu.make_async_copy(hid.at[0:1], first_hbm, sems.at[0]),
        pltpu.make_async_copy(hid.at[3:4], last_hbm, sems.at[1]),
        pltpu.make_async_copy(hid, hid_hbm, sems.at[2]),
    ]
    for put in puts:
        put.start()
    mean, off = local_moments(full, 4)
    line = turned(jnp.concatenate([mean, off], axis=0))[0:1, :]
    line = jnp.concatenate([line, jnp.zeros((1, 64), f32)], axis=1)
    for d in range(GROUPS):
        st_ref[d] = line
    for put in puts:
        put.wait()


WT = (CU, 3 * ROWK)
CONV_SCRATCH = [
    MANY,
    pltpu.VMEM((GROUPS * 32, 128), f32),
    pltpu.VMEM((DEPTH, 128), bf16),
    pltpu.VMEM(WT, bf16),
]


def conv1(flags, own, wto, other, act, shift):
    edge = pltpu.HBM((1, CU, WIDTH), bf16)
    return pl.pallas_call(
        conv1_kernel,
        out_shape=(
            pltpu.HBM((4, CU, WIDTH), bf16),
            edge,
            edge,
            jax.ShapeDtypeStruct((GROUPS, 1, 128), f32),
        ),
        in_specs=[SCALARS] + [WHOLE] * 5,
        out_specs=(FAR, FAR, FAR, WHOLE),
        scratch_shapes=CONV_SCRATCH
        + [
            pltpu.VMEM((8 * CU, 128), f32),
            pltpu.VMEM((4, CU, WIDTH), bf16),
            pltpu.SemaphoreType.DMA((3,)),
        ],
        compiler_params=PARAMS,
        cost_estimate=cost(5),
        name="conv1",
    )(flags, *near(own, wto, other, act), shift.reshape(1, CU))


def own2_kernel(own_ref, wt_ref, many):
    own_block(own_ref, many, wt_ref)


def own2_part(own):
    return pl.pallas_call(
        own2_kernel,
        out_shape=pltpu.VMEM((128, 3 * ROWK), bf16),
        in_specs=[WHOLE],
        out_specs=WHOLE,
        scratch_shapes=[MANY],
        compiler_params=PARAMS,
        cost_estimate=cost(1),
        name="own2",
    )(*near(own))


def conv2_kernel(flags_ref, own_ref, wto_ref, other_ref, act_ref, bias_ref, x_ref, out_ref, many, many2, w, wt):
    all_weights(flags_ref, own_ref, wto_ref, other_ref, many, many2, w, wt)
    bias = column_of(bias_ref[...])
    bias = jnp.concatenate([bias, bias], axis=1)
    for h in range(4):
        out_ref[h] = (x_ref[h].astype(f32) + (conv_row(h, act_ref, wt) + bias)).astype(bf16)


def conv2(flags, own, wto, other, act, bias, x):
    return pl.pallas_call(
        conv2_kernel,
        out_shape=jax.ShapeDtypeStruct((4, CU, WIDTH), bf16),
        in_specs=[SCALARS] + [WHOLE] * 6,
        out_specs=WHOLE,
        scratch_shapes=CONV_SCRATCH,
        compiler_params=PARAMS,
        cost_estimate=cost(4),
        name="conv2",
    )(flags, *near(own, wto, other, act), bias.reshape(1, CU), *near(x))


def to_all(chunks, axis):
    return lax.all_to_all(chunks, axis, 0, 0, tiled=True)


def swapped(chunks):
    return lax.ppermute(chunks, "core", [(0, 1), (1, 0)])


def edges(first, last):
    count = lax.axis_size(ROW)
    above = lax.ppermute(last, ROW, [(i, i + 1) for i in range(count - 1)])
    below = lax.ppermute(first, ROW, [(i + 1, i) for i in range(count - 1)])
    return above, below


def block_of(
    lat_pixels,
    first_gain,
    first_beta,
    first_kernel,
    time_shift,
    second_gain,
    second_beta,
    second_kernel,
    second_bias,
):
    x = lat_pixels.transpose(0, 2, 1)
    place = lax.axis_index(ROW)
    last = lax.axis_size(ROW) - 1
    flags = jnp.stack(
        [lax.axis_index("core"), (place > 0).astype(jnp.int32), (place < last).astype(jnp.int32), place % XS]
    ).astype(jnp.int32)
    chunks = prep(flags, x, first_kernel.transpose(0, 2, 1, 3), second_kernel.transpose(0, 2, 1, 3))
    got = to_all(chunks, "row_0")
    above, below = edges(x[0:1], x[3:4])
    xch, w2z = middle(got, above, below)
    own1 = to_all(xch, "row_1")
    pieces = [w2z]
    for s in range(1, XS):
        pieces.append(lax.ppermute(w2z, "row_1", [(i, (i + s) % XS) for i in range(XS)]))
    other1 = swapped(own1)
    act, wto = norm1(flags, own1, above, x, below, first_gain, first_beta)
    hidden, first, last, st = conv1(flags, own1, wto, other1, act, time_shift)
    stats = to_all(st, ROW)
    habove, hbelow = edges(first, last)
    own2 = join(flags, pieces, st)
    other2 = swapped(own2)
    wto2 = own2_part(own2)
    act2 = norm2(flags, stats, habove, hidden, hbelow, second_gain, second_beta)
    out = conv2(flags, own2, wto2, other2, act2, second_bias, x)
    return out.transpose(0, 2, 1)


def solution(mesh):
    split = Mesh(mesh.devices.reshape(mesh.shape["img"] // 2, 2, 8, 4), ("y", "core", "row_0", "row_1"))
    placed = (
        P(IMG_ROW, None, None),
        P(),
        P(),
        P(None, None, ROW, None),
        P(("y", "core")),
        P(),
        P(),
        P(None, None, ROW, None),
        P(),
    )
    return jax.shard_map(block_of, mesh=split, in_specs=placed, out_specs=P(IMG_ROW, None, None), check_vma=False)
```

```python
import jax
import jax.numpy as jnp
from jax import lax
from jax.experimental import pallas as pl
from jax.experimental.pallas import tpu as pltpu
from jax.sharding import Mesh
from jax.sharding import PartitionSpec as P

GROUPS = 32
PER = 10
CU = 320
WIDTH = 256
TAPS = 9
SLABS = TAPS * PER
PAIRS = SLABS // 2
CROWS = 23
CHUNK = 120
ZS, XS = 8, 4
LOCAL = 4.0 * PER * WIDTH
DEPTH = SLABS * GROUPS
ROWK = 1024
ROW = ("row_0", "row_1")
IMG_ROW = ("y", "core", "row_0", "row_1")
EPS = 1e-06

f32 = jnp.float32
bf16 = jnp.bfloat16
ANYWHERE = pl.BlockSpec(memory_space=pl.ANY)
FAR = pl.BlockSpec(memory_space=pltpu.HBM)
WHOLE = pl.BlockSpec(memory_space=pltpu.VMEM)
SCALARS = pl.BlockSpec(memory_space=pltpu.SMEM)
PARAMS = pltpu.CompilerParams(vmem_limit_bytes=24 * 1024 * 1024)


def far(array):
    return pltpu.with_memory_space_constraint(array, pltpu.HBM)


def near(*arrays):
    return [pltpu.with_memory_space_constraint(a, pltpu.VMEM) for a in arrays]


def cost(us):
    return pl.CostEstimate(flops=int(us * 2e8), bytes_accessed=1 << 20, transcendentals=0)


def widen(ref, at, values):
    ref[at : at + CU, :] = values[:, 0:128]
    ref[at + CU : at + 2 * CU, :] = values[:, 128:256]


def slab_of(ref, j, row=0):
    at = row * 2 * CU + j
    halves = [ref[pl.ds(at + n * CU, GROUPS, stride=PER), :] for n in range(2)]
    return jnp.concatenate(halves, axis=1)


def same_slab(ref, j):
    half = ref[pl.ds(j, GROUPS, stride=PER), :]
    return jnp.concatenate([half, half], axis=1)


def local_moments(values, rows):
    total = jnp.zeros((GROUPS, WIDTH), f32)
    for h in range(rows):
        for j in range(PER):
            total += slab_of(values, j, h)
    mean = jnp.sum(total, axis=1, keepdims=True) * (1.0 / (rows * PER * WIDTH))
    off = jnp.zeros((GROUPS, WIDTH), f32)
    for h in range(rows):
        for j in range(PER):
            d = slab_of(values, j, h) - mean
            off += d * d
    return mean, jnp.sum(off, axis=1, keepdims=True)


def turned(column):
    return jnp.transpose(jnp.broadcast_to(column, (column.shape[0], 128)))


def in_three(v):
    hi = v.astype(bf16).astype(f32)
    rest = v - hi
    mid = rest.astype(bf16).astype(f32)
    return hi, mid, rest - mid


def prep_kernel(
    flags_ref, x_hbm, w_hbm, w2_hbm, ch_ref, x_ref, w_ref, w2_ref, wide, flat, chunk, x_sem, w_sem, w2_sem
):
    core = flags_ref[0]
    get_x = pltpu.make_async_copy(x_hbm, x_ref, x_sem)
    get_w = pltpu.make_async_copy(w_hbm, w_ref, w_sem)
    get_w2 = pltpu.make_async_copy(w2_hbm, w2_ref, w2_sem)
    get_w.start()
    get_w2.start()
    get_x.start()
    get_w2.wait()
    fill_chunk(core, w2_ref, flat, chunk)
    whole = chunk[...].astype(bf16)
    for d in range(ZS):
        ch_ref[d, CHUNK : 2 * CHUNK] = whole
    get_w.wait()
    fill_chunk(core, w_ref, flat, chunk)
    get_x.wait()
    for h in range(4):
        widen(wide, h * 2 * CU, x_ref[h].astype(f32))
    mean, off = local_moments(wide, 4)
    rows = [turned(col)[0:1, :] for col in (mean, off)]
    put_stats(rows, chunk)
    whole = chunk[...].astype(bf16)
    for d in range(ZS):
        ch_ref[d, 0:CHUNK] = whole


def put_stats(rows, chunk):
    for k, row in enumerate(rows):
        for n, piece in enumerate(in_three(row[:, 0:GROUPS])):
            at = SLABS + CROWS + 3 * k + n
            chunk[at : at + 1, 0:GROUPS] = piece


def got_stats(tail):
    piece = lambda n: tail[:, n, 0:GROUPS]
    return piece(1) + piece(2) + piece(3), piece(4) + piece(5) + piece(6)


def pooled(means, offs, count):
    n = means.shape[0]
    mean = jnp.sum(means, axis=0, keepdims=True) * (1.0 / n)
    d = means - mean
    return mean, jnp.sum(offs, axis=0, keepdims=True) + count * jnp.sum(d * d, axis=0, keepdims=True)


def middle_kernel(g_ref, above_ref, below_ref, xch_hbm, w2_ref, tail, first, sems):
    puts = [
        pltpu.make_async_copy(g_ref.at[1:ZS, 0:CHUNK], xch_hbm.at[d, 1:ZS], sems.at[0, d]) for d in range(XS)
    ]
    for put in puts:
        put.start()
    rows = pooled(*got_stats(g_ref[:, CHUNK - 8 : CHUNK, :].astype(f32)), LOCAL)
    tail[...] = g_ref[0, 0:CHUNK, :].astype(f32)
    put_stats(rows, tail)
    first[...] = tail[...].astype(bf16)
    for d in range(XS):
        puts.append(pltpu.make_async_copy(first, xch_hbm.at[d, 0], sems.at[1, d]))
        puts[-1].start()
    for z in range(ZS):
        w2_ref[z] = g_ref[z, CHUNK : 2 * CHUNK, :]
    for put in puts:
        put.wait()


def middle(got, above, below):
    return pl.pallas_call(
        middle_kernel,
        out_shape=(
            pltpu.HBM((XS, ZS, CHUNK, 128), bf16),
            pltpu.VMEM((ZS, CHUNK, 128), bf16),
        ),
        in_specs=[WHOLE, ANYWHERE, ANYWHERE],
        out_specs=(FAR, WHOLE),
        scratch_shapes=[
            pltpu.VMEM((CHUNK, 128), f32),
            pltpu.VMEM((CHUNK, 128), bf16),
            pltpu.SemaphoreType.DMA((2, XS)),
        ],
        compiler_params=PARAMS,
        cost_estimate=cost(1),
        name="middle",
    )(*near(got), above, below)


def join_kernel(flags_ref, own_ref, a_ref, b_ref, c_ref, after_ref, out_ref):
    x = flags_ref[3]
    for s, ref in enumerate((own_ref, a_ref, b_ref, c_ref)):
        at = (x + XS - s) % XS
        for z in range(ZS):
            out_ref[z * XS + at] = ref[z]


def join(flags, pieces, after):
    return pl.pallas_call(
        join_kernel,
        out_shape=pltpu.VMEM((GROUPS, CHUNK, 128), bf16),
        in_specs=[SCALARS] + [WHOLE] * 4 + [ANYWHERE],
        out_specs=WHOLE,
        compiler_params=PARAMS,
        cost_estimate=cost(1),
        name="join",
    )(flags, *near(*pieces), after)


def fill_chunk(core, w_ref, flat, chunk):
    for p in range(3):
        for j in range(PER):
            at = (p * PER + j) * 3
            flat[at : at + 3, 0:CU] = w_ref[p, j].astype(f32)
    chunk[...] = jnp.zeros((CHUNK, 128), f32)
    first = core == 0
    chunk[0:SLABS, :] = jnp.where(first, flat[0:SLABS, 0:128], flat[0:SLABS, 128:256])
    for c in range(2):
        t0 = (CROWS - 1) * c
        lo = flat[t0 : t0 + CROWS, 256:384]
        hi = pltpu.roll(flat[PAIRS + t0 : PAIRS + t0 + CROWS, 256:384], 64, 1)
        lane = lax.broadcasted_iota(jnp.int32, (CROWS, 128), 1)
        both = jnp.where(lane < 64, lo, hi)

        @pl.when(core == c)
        def _():
            chunk[SLABS : SLABS + CROWS, :] = both


def prep(flags, *arrays):
    arrays = [far(a) for a in arrays]
    return pl.pallas_call(
        prep_kernel,
        out_shape=jax.ShapeDtypeStruct((ZS, 2 * CHUNK, 128), bf16),
        in_specs=[SCALARS] + [FAR] * 3,
        out_specs=WHOLE,
        scratch_shapes=[
            pltpu.VMEM((4, CU, WIDTH), bf16),
            pltpu.VMEM((3, PER, 3, CU), bf16),
            pltpu.VMEM((3, PER, 3, CU), bf16),
            pltpu.VMEM((8 * CU, 128), f32),
            pltpu.VMEM((96, 384), f32),
            pltpu.VMEM((CHUNK, 128), f32),
            pltpu.SemaphoreType.DMA,
            pltpu.SemaphoreType.DMA,
            pltpu.SemaphoreType.DMA,
        ],
        compiler_params=PARAMS,
        cost_estimate=cost(3),
        name="prep",
    )(flags, *arrays)


def column_of(row):
    return jnp.transpose(jnp.broadcast_to(row, (128, row.shape[1])))


def combine(means, offs, count):
    center, off = pooled(means, offs, count)
    inv = lax.rsqrt(off * (1.0 / (means.shape[0] * count)) + EPS)
    return column_of(center), column_of(inv)


def activate(flags_ref, rows, center, inv, gain_ref, beta_ref, cols, wide, act_ref):
    gains, betas = cols
    gains[...] = column_of(gain_ref[...])
    betas[...] = column_of(beta_ref[...])
    two = lambda a: jnp.concatenate([a, a], axis=1)
    center, inv = two(center), two(inv)
    lane = lax.broadcasted_iota(jnp.int32, (GROUPS, WIDTH), 1)
    for h in (1, 2, 3, 4, 0, 5):
        act_ref[h * ROWK + 3 * CU : (h + 1) * ROWK, :] = jnp.zeros((ROWK - 3 * CU, WIDTH), bf16)
        widen(wide, 0, rows(h).astype(f32))
        for j in range(PER):
            v = (slab_of(wide, j) - center) * inv
            v = v * same_slab(gains, j) + same_slab(betas, j)
            v = v / (1.0 + jnp.exp(-v))
            if h == 0:
                v = jnp.where(flags_ref[1] == 0, 0.0, v)
            if h == 5:
                v = jnp.where(flags_ref[2] == 0, 0.0, v)
            left = jnp.where(lane == 0, 0.0, pltpu.roll(v, 1, 1))
            right = jnp.where(lane == WIDTH - 1, 0.0, pltpu.roll(v, WIDTH - 1, 1))
            at = h * ROWK + j * 3 * GROUPS
            act_ref[at : at + GROUPS, :] = left.astype(bf16)
            act_ref[at + GROUPS : at + 2 * GROUPS, :] = v.astype(bf16)
            act_ref[at + 2 * GROUPS : at + 3 * GROUPS, :] = right.astype(bf16)


def fetched(fars, here, sems):
    copies = [pltpu.make_async_copy(far_ref, here.at[n], sems.at[n]) for n, far_ref in enumerate(fars)]
    for copy in copies:
        copy.start()

    def get(n):
        copies[n].wait()
        return here[n]

    return get


def norm1_kernel(
    flags_ref, g_ref, top_hbm, mid_ref, bot_hbm, gain_ref, beta_ref, act_ref, wt_ref, gains, betas, wide, many, here, sems
):
    edge = fetched((top_hbm.at[0], bot_hbm.at[0]), here, sems)
    own_block(g_ref, many, wt_ref)
    center, inv = combine(*got_stats(g_ref[:, 0, CHUNK - 8 : CHUNK, :].astype(f32)), ZS * LOCAL)
    rows = lambda h: mid_ref[h - 1] if 0 < h < 5 else edge(int(h == 5))
    activate(flags_ref, rows, center, inv, gain_ref, beta_ref, (gains, betas), wide, act_ref)


def norm2_kernel(
    flags_ref, s_ref, top_hbm, mid_hbm, bot_hbm, gain_ref, beta_ref, act_ref, gains, betas, wide, here, sems
):
    row = fetched([mid_hbm.at[h] for h in range(4)] + [top_hbm.at[0], bot_hbm.at[0]], here, sems)
    both = s_ref[:, 0, :]
    center, inv = combine(both[:, 0:GROUPS], both[:, GROUPS : 2 * GROUPS], LOCAL)
    rows = lambda h: row(h - 1 if 0 < h < 5 else 5 if h else 4)
    activate(flags_ref, rows, center, inv, gain_ref, beta_ref, (gains, betas), wide, act_ref)


NORM_SCRATCH = [
    pltpu.VMEM((CU, 128), f32),
    pltpu.VMEM((CU, 128), f32),
    pltpu.VMEM((2 * CU, 128), f32),
]
MANY = pltpu.VMEM((GROUPS * CHUNK, 128), f32)
ACT = pltpu.VMEM((6 * ROWK, WIDTH), bf16)


def rows_here(n):
    return [pltpu.VMEM((n, CU, WIDTH), bf16), pltpu.SemaphoreType.DMA((n,))]


def norm1(flags, own, top, mid, bot, gain, beta):
    return pl.pallas_call(
        norm1_kernel,
        out_shape=(ACT, pltpu.VMEM((128, 3 * ROWK), bf16)),
        in_specs=[SCALARS, WHOLE, FAR, WHOLE, FAR, WHOLE, WHOLE],
        out_specs=(WHOLE, WHOLE),
        scratch_shapes=NORM_SCRATCH + [MANY] + rows_here(2),
        compiler_params=PARAMS,
        cost_estimate=cost(3),
        name="norm1",
    )(flags, *near(own), far(top), mid, far(bot), gain.reshape(1, CU), beta.reshape(1, CU))


def norm2(flags, stats, top, mid, bot, gain, beta):
    return pl.pallas_call(
        norm2_kernel,
        out_shape=ACT,
        in_specs=[SCALARS, WHOLE, FAR, FAR, FAR, WHOLE, WHOLE],
        out_specs=WHOLE,
        scratch_shapes=NORM_SCRATCH + rows_here(6),
        compiler_params=PARAMS,
        cost_estimate=cost(2),
        name="norm2",
    )(flags, stats, far(top), far(mid), far(bot), gain.reshape(1, CU), beta.reshape(1, CU))


def shard_at(g_ref, d, rows):
    part = g_ref[d, rows, :] if len(g_ref.shape) == 3 else g_ref[d % XS, d // XS, rows, :]
    return part.astype(f32)


def spread_out(g_ref, many):
    for d in range(GROUPS):
        many[d * CHUNK : (d + 1) * CHUNK, :] = shard_at(g_ref, d, slice(0, CHUNK))


def block(many):
    out = []
    for p in range(3):
        slabs = [many[pl.ds(p * 30 + m, GROUPS, stride=CHUNK), :].astype(bf16) for m in range(30)]
        slabs.append(jnp.zeros((ROWK - 3 * CU, 128), bf16))
        out.append(jnp.transpose(jnp.concatenate(slabs, axis=0)))
    return out


def own_block(g_ref, many, wt_ref):
    spread_out(g_ref, many)
    for p, part in enumerate(block(many)):
        wt_ref[:, p * ROWK : (p + 1) * ROWK] = part


def rest_of(core, many, w):
    t0 = core * (CROWS - 1)
    for t in range(CROWS):
        v = many[pl.ds(SLABS + t, GROUPS, stride=CHUNK), :]
        at = pl.multiple_of((t0 + t) * GROUPS, GROUPS)
        w[pl.ds(at, GROUPS), :] = v.astype(bf16)
        w[pl.ds(at + PAIRS * GROUPS, GROUPS), :] = pltpu.roll(v, 64, 1).astype(bf16)


def rest_turned(w, wt):
    for p in range(3):
        part = jnp.concatenate([w[p * 3 * CU : (p + 1) * 3 * CU, :], jnp.zeros((ROWK - 3 * CU, 128), bf16)], axis=0)
        wt[128:192, p * ROWK : (p + 1) * ROWK] = jnp.transpose(part)[0:64, :]


def conv(h, act_ref, w):
    return jnp.dot(w[...], act_ref[h * ROWK : (h + 3) * ROWK, :], preferred_element_type=f32)


def all_weights(flags_ref, own_ref, other_ref, many, many2, w, wt):
    core = flags_ref[0]
    for d in range(GROUPS):
        many2[d * 32 : (d + 1) * 32, :] = shard_at(own_ref, d, slice(CHUNK - 32, CHUNK))
    t0 = core * (CROWS - 1)
    for t in range(CROWS):
        v = many2[pl.ds(2 + t, GROUPS, stride=32), :]
        at = pl.multiple_of((t0 + t) * GROUPS, GROUPS)
        w[pl.ds(at, GROUPS), :] = v.astype(bf16)
        w[pl.ds(at + PAIRS * GROUPS, GROUPS), :] = pltpu.roll(v, 64, 1).astype(bf16)
    spread_out(other_ref, many)
    rest_of(1 - core, many, w)
    rest_turned(w, wt)
    for p, part in enumerate(block(many)):
        wt[0:128, p * ROWK : (p + 1) * ROWK] = part


def convolve(flags_ref, own_ref, wto_ref, other_ref, act_ref, many, many2, w, wt, put):
    core = flags_ref[0]
    for h in range(4):
        put(h, pl.multiple_of(core * 128, 128), 128, conv(h, act_ref, wto_ref))
    all_weights(flags_ref, own_ref, other_ref, many, many2, w, wt)
    for h in range(4):
        both = conv(h, act_ref, wt)
        put(h, pl.multiple_of((1 - core) * 128, 128), 128, both[0:128])
        put(h, 256, 64, both[128:192])


def conv1_kernel(
    flags_ref, own_ref, wto_ref, other_ref, act_ref, shift_ref, hid_hbm, first_hbm, last_hbm, st_ref, many, many2, w, wt, cols, full, hid, sems
):
    cols[...] = column_of(shift_ref[...])

    def put(h, start, size, part):
        add = cols[pl.ds(start, size), :]
        row = (part + jnp.concatenate([add, add], axis=1)).astype(bf16)
        hid[h, pl.ds(start, size), :] = row
        for n in range(2):
            at = start + (2 * h + n) * CU
            at = at if isinstance(at, int) else pl.multiple_of(at, 64)
            full[pl.ds(at, size), :] = row[:, n * 128 : (n + 1) * 128].astype(f32)

    convolve(flags_ref, own_ref, wto_ref, other_ref, act_ref, many, many2, w, wt, put)
    puts = [
        pltpu.make_async_copy(hid.at[0:1], first_hbm, sems.at[0]),
        pltpu.make_async_copy(hid.at[3:4], last_hbm, sems.at[1]),
        pltpu.make_async_copy(hid, hid_hbm, sems.at[2]),
    ]
    for put in puts:
        put.start()
    mean, off = local_moments(full, 4)
    line = turned(jnp.concatenate([mean, off], axis=0))[0:1, :]
    line = jnp.concatenate([line, jnp.zeros((1, 64), f32)], axis=1)
    for d in range(GROUPS):
        st_ref[d] = line
    for put in puts:
        put.wait()


WT = (CU - 128, 3 * ROWK)
CONV_SCRATCH = [
    MANY,
    pltpu.VMEM((GROUPS * 32, 128), f32),
    pltpu.VMEM((DEPTH, 128), bf16),
    pltpu.VMEM(WT, bf16),
    pltpu.VMEM((CU, 128), f32),
]


def conv1(flags, own, wto, other, act, shift):
    edge = pltpu.HBM((1, CU, WIDTH), bf16)
    return pl.pallas_call(
        conv1_kernel,
        out_shape=(
            pltpu.HBM((4, CU, WIDTH), bf16),
            edge,
            edge,
            jax.ShapeDtypeStruct((GROUPS, 1, 128), f32),
        ),
        in_specs=[SCALARS] + [WHOLE] * 5,
        out_specs=(FAR, FAR, FAR, WHOLE),
        scratch_shapes=CONV_SCRATCH
        + [
            pltpu.VMEM((8 * CU, 128), f32),
            pltpu.VMEM((4, CU, WIDTH), bf16),
            pltpu.SemaphoreType.DMA((3,)),
        ],
        compiler_params=PARAMS,
        cost_estimate=cost(5),
        name="conv1",
    )(flags, *near(own, wto, other, act), shift.reshape(1, CU))


def own2_kernel(own_ref, wt_ref, many):
    own_block(own_ref, many, wt_ref)


def own2_part(own):
    return pl.pallas_call(
        own2_kernel,
        out_shape=pltpu.VMEM((128, 3 * ROWK), bf16),
        in_specs=[WHOLE],
        out_specs=WHOLE,
        scratch_shapes=[MANY],
        compiler_params=PARAMS,
        cost_estimate=cost(1),
        name="own2",
    )(*near(own))


def conv2_kernel(flags_ref, own_ref, wto_ref, other_ref, act_ref, bias_ref, x_ref, out_ref, many, many2, w, wt, cols):
    cols[...] = column_of(bias_ref[...])

    def put(h, start, size, part):
        at = pl.ds(start, size)
        add = cols[at, :]
        total = x_ref[h, at, :].astype(f32) + (part + jnp.concatenate([add, add], axis=1))
        out_ref[h, at, :] = total.astype(bf16)

    convolve(flags_ref, own_ref, wto_ref, other_ref, act_ref, many, many2, w, wt, put)


def conv2(flags, own, wto, other, act, bias, x):
    return pl.pallas_call(
        conv2_kernel,
        out_shape=jax.ShapeDtypeStruct((4, CU, WIDTH), bf16),
        in_specs=[SCALARS] + [WHOLE] * 6,
        out_specs=WHOLE,
        scratch_shapes=CONV_SCRATCH,
        compiler_params=PARAMS,
        cost_estimate=cost(4),
        name="conv2",
    )(flags, *near(own, wto, other, act), bias.reshape(1, CU), *near(x))


def to_all(chunks, axis):
    return lax.all_to_all(chunks, axis, 0, 0, tiled=True)


def swapped(chunks):
    return lax.ppermute(chunks, "core", [(0, 1), (1, 0)])


def edges(first, last):
    count = lax.axis_size(ROW)
    above = lax.ppermute(last, ROW, [(i, i + 1) for i in range(count - 1)])
    below = lax.ppermute(first, ROW, [(i + 1, i) for i in range(count - 1)])
    return above, below


def block_of(
    lat_pixels,
    first_gain,
    first_beta,
    first_kernel,
    time_shift,
    second_gain,
    second_beta,
    second_kernel,
    second_bias,
):
    x = lat_pixels.transpose(0, 2, 1)
    place = lax.axis_index(ROW)
    last = lax.axis_size(ROW) - 1
    flags = jnp.stack(
        [lax.axis_index("core"), (place > 0).astype(jnp.int32), (place < last).astype(jnp.int32), place % XS]
    ).astype(jnp.int32)
    chunks = prep(flags, x, first_kernel.transpose(0, 2, 1, 3), second_kernel.transpose(0, 2, 1, 3))
    got = to_all(chunks, "row_0")
    above, below = edges(x[0:1], x[3:4])
    xch, w2z = middle(got, above, below)
    own1 = to_all(xch, "row_1")
    pieces = [w2z]
    for s in range(1, XS):
        pieces.append(lax.ppermute(w2z, "row_1", [(i, (i + s) % XS) for i in range(XS)]))
    other1 = swapped(own1)
    act, wto = norm1(flags, own1, above, x, below, first_gain, first_beta)
    hidden, first, last, st = conv1(flags, own1, wto, other1, act, time_shift)
    stats = to_all(st, ROW)
    habove, hbelow = edges(first, last)
    own2 = join(flags, pieces, st)
    other2 = swapped(own2)
    wto2 = own2_part(own2)
    act2 = norm2(flags, stats, habove, hidden, hbelow, second_gain, second_beta)
    out = conv2(flags, own2, wto2, other2, act2, second_bias, x)
    return out.transpose(0, 2, 1)


def solution(mesh):
    split = Mesh(mesh.devices.reshape(mesh.shape["img"] // 2, 2, 8, 4), ("y", "core", "row_0", "row_1"))
    placed = (
        P(IMG_ROW, None, None),
        P(),
        P(),
        P(None, None, ROW, None),
        P(("y", "core")),
        P(),
        P(),
        P(None, None, ROW, None),
        P(),
    )
    return jax.shard_map(block_of, mesh=split, in_specs=placed, out_specs=P(IMG_ROW, None, None), check_vma=False)
```
